16 devices in a mesh: dp: 2 (over y, z), tp: 8 (over x, core).
Axes of the slice: x: 4, y: 2, z: 1, core: 2. Of those that a mesh axis runs over, the one named last changes fastest.
The devices are a block of a 4x4x8 slice.
Arguments:
- x: bfloat16 [4096, 7168], P(('dp', 'tp')), parts along dimension 0
- gain: bfloat16 [7168], replicated
- wq: bfloat16 [7168, 7168], P(None, 'tp')
- wk: bfloat16 [7168, 1024], P(None, 'tp')
- wv: bfloat16 [7168, 1024], P(None, 'tp')
- wo: bfloat16 [7168, 7168], P('tp')
Outputs:
- output: bfloat16 [4096, 7168], P(('dp', 'tp')), parts along dimension 0
There are 2 independent parts. The reference program is written for one: setup_inputs(seed, part) draws one part's arguments, and reference() takes and returns one part's arrays. A program takes and returns all parts, laid end to end along the dimension named above; an argument that names none is the same for every part.
All inputs are finite; a program needn't handle non-finite values.
Results may differ from the reference program's by a relative error of at most 0.012.
Values are sent between devices in bfloat16 or wider.
A program may use at most 768 MiB of HBM per device.

```python
import jax
import jax.numpy as jnp
from jax import lax

ROWS = 2048
D = 7168
HEADS = 56
KV_HEADS = 8
HEAD = 128
THETA = 10000


def setup_inputs(seed: int = 0, part: int = 0) -> dict:
    kx, kn, kq, kk, kv, ko = jax.random.split(jax.random.key(seed), 6)

    def weights(key, rows, columns):
        return jax.random.normal(key, (rows, columns), jnp.float32) * rows**-0.5

    drawn = {
        "x": jax.random.normal(jax.random.fold_in(kx, part), (ROWS, D), jnp.float32),
        "gain": 1 + 0.1 * jax.random.normal(kn, (D,), jnp.float32),
        "wq": 2 * weights(kq, D, HEADS * HEAD),
        "wk": 2 * weights(kk, D, KV_HEADS * HEAD),
        "wv": 4 * weights(kv, D, KV_HEADS * HEAD),
        "wo": weights(ko, HEADS * HEAD, D),
    }
    return {k: v.astype(jnp.bfloat16) for k, v in drawn.items()}


def normed(x, gain):
    wide = x.astype(jnp.float32)
    scale = lax.rsqrt(jnp.mean(wide * wide, -1, keepdims=True) + 1e-6)
    return (wide * scale * gain.astype(jnp.float32)).astype(jnp.bfloat16)


def turned(t, place, theta):
    half = t.shape[-1] // 2
    angle = place.astype(jnp.float32)[:, None] * theta ** (-jnp.arange(half, dtype=jnp.float32) / half)
    cos, sin = jnp.cos(angle)[:, None], jnp.sin(angle)[:, None]
    a, b = t[..., :half].astype(jnp.float32), t[..., half:].astype(jnp.float32)
    return jnp.concatenate([a * cos - b * sin, b * cos + a * sin], -1).astype(jnp.bfloat16)


def matmul(a, w):
    return jnp.dot(a, w, preferred_element_type=jnp.float32).astype(jnp.bfloat16)


def einsum(form, a, b):
    return jnp.einsum(form, a.astype(jnp.float32), b.astype(jnp.float32))


def attention(q, k, v):
    scores = einsum("tgsd,ugd->gstu", q, k) * q.shape[-1] ** -0.5
    token = jnp.arange(q.shape[0])
    scores = jnp.where(token[:, None] >= token, scores, -jnp.inf)
    weights = jax.nn.softmax(scores, -1).astype(jnp.bfloat16)
    return einsum("gstu,ugd->tgsd", weights, v).astype(jnp.bfloat16)


def reference(x, gain, wq, wk, wv, wo):
    a, place = normed(x, gain), jnp.arange(ROWS)
    q = turned(matmul(a, wq).reshape(ROWS, HEADS, HEAD), place, THETA).reshape(ROWS, KV_HEADS, -1, HEAD)
    k = turned(matmul(a, wk).reshape(ROWS, KV_HEADS, HEAD), place, THETA)
    v = matmul(a, wv).reshape(ROWS, KV_HEADS, HEAD)
    seen = attention(q, k, v).reshape(ROWS, HEADS * HEAD)
    return (x.astype(jnp.float32) + jnp.dot(seen, wo, preferred_element_type=jnp.float32)).astype(jnp.bfloat16)
```

```python
import functools

import jax
import jax.numpy as jnp
import numpy as np
from jax import lax
from jax.experimental import pallas as pl
from jax.experimental.pallas import tpu as pltpu
from jax.sharding import PartitionSpec as P

HEAD = 128
THETA = 10000
NEG = -1e30
HIDDEN = 2 * NEG
LOG2E = 1.4426950408889634
VMEM = 67043328
CORES = 2
CHIPS = 4
WIDE = 256
TILE = 512
KEYS = 512
LAG = 6
SLOTS = 8


def _dot(a, b, ca, cb):
    return lax.dot_general(a, b, (((ca,), (cb,)), ((), ())), preferred_element_type=jnp.float32)


def _places():
    me = lax.axis_index("tp")
    chip, core = me // CORES, lax.rem(me, CORES)
    right = lax.rem(chip + 1, CHIPS) * CORES + core
    left = lax.rem(chip + CHIPS - 1, CHIPS) * CORES + core
    return chip, core, right, left, chip * CORES + 1 - core


def _greet(peers):
    barrier = pltpu.get_barrier_semaphore()
    for peer in peers:
        pl.semaphore_signal(barrier, inc=1, device_id={"tp": peer}, device_id_type=pl.DeviceIdType.MESH)
    return lambda: pl.semaphore_wait(barrier, len(peers))


def _send(src, dst, send_sem, recv_sem, device):
    return pltpu.make_async_remote_copy(src_ref=src, dst_ref=dst, send_sem=send_sem, recv_sem=recv_sem, device_id={"tp": device},
                                        device_id_type=pl.DeviceIdType.MESH)


def _gather(x_ref, gain_ref, trig_ref, wq_ref, wk_ref, wv_ref, qk_ref, v_ref, xs, w, w_last, trig, x_sem, w_sem, right_s, right_r, left_s,
            left_r, own_s, own_r, pass_s, pass_r):
    chip, core, right, left, partner = _places()
    ready = _greet((right, left, partner))
    rows = xs.shape[1]
    piece = rows // 4
    heads = qk_ref.shape[0]

    def at(group, slot):
        return xs.at[group, pl.ds(slot * piece, piece)]

    loads = [pltpu.make_async_copy(x_ref.at[pl.ds(p * piece, piece)], at(core, p), x_sem.at[p]) for p in range(4)]
    for p in (0, 2, 1, 3):
        loads[p].start()
    n_q = wq_ref.shape[1]
    blocks = []
    for n in range(n_q // WIDE):
        blocks.append((wq_ref.at[:, n * WIDE : (n + 1) * WIDE], w.at[n]))
    blocks.append((wq_ref.at[:, n_q // WIDE * WIDE :], w.at[n_q // WIDE, :, : WIDE - HEAD]))
    blocks.append((wk_ref, w.at[n_q // WIDE, :, WIDE - HEAD :]))
    blocks.append((wv_ref, w_last))
    blocks.append((trig_ref, trig))
    fetches = [pltpu.make_async_copy(a, b, w_sem.at[n]) for n, (a, b) in enumerate(blocks)]
    for f in fetches:
        f.start()

    def norm(p):
        def body(i, _):
            here = pl.ds(p * piece + i * 16, 16)
            wide = xs[core, here, :].astype(jnp.float32)
            scale = lax.rsqrt(jnp.mean(wide * wide, -1, keepdims=True) + 1e-6)
            xs[core, here, :] = (wide * scale * gain_ref[...].astype(jnp.float32)).astype(jnp.bfloat16)

        lax.fori_loop(0, piece // 16, body, None)

    def go_right(k, src):
        return _send(src, at(2 + k, core), right_s.at[k], right_r.at[k], right)

    def go_left(k, src):
        return _send(src, at(2 + k, 2 + core), left_s.at[k], left_r.at[k], left)

    def over_own(p):
        return _send(at(core, p), at(core, p), own_s.at[p], own_r.at[p], partner)

    def over(k, side):
        slot = 2 * side + core
        return _send(at(2 + k, slot), at(2 + k, slot), pass_s.at[side, k], pass_r.at[side, k], partner)

    def own_right(k):
        return go_right(k, at(core, k))

    def own_left(k):
        return go_left(k, at(core, (k + 2) % 4))

    for i, p in enumerate((0, 2, 1, 3)):
        loads[p].wait()
        norm(p)
        if i == 0:
            ready()
        if p < 2:
            own_right(p).start()
        else:
            own_left(p - 2).start()
        over_own(p).start()
    for k in (2, 3):
        own_right(k).start()
        own_left(k).start()
    for f in fetches:
        f.wait()

    def token(group, slot):
        k = group - 2
        low = slot < 2
        device = CORES * chip + group
        part = slot
        near = lax.rem(chip + (CHIPS - 1 if low else 1), CHIPS) * CORES + slot % 2
        far = lax.rem(chip + 2, CHIPS) * CORES + slot % 2
        near_part = k if low else lax.rem(k + 2, 4)
        far_part = k - 4 + (0 if low else 2)
        device = jnp.where(group < 2, device, jnp.where(group < 6, near, far))
        part = jnp.where(group < 2, part, jnp.where(group < 6, near_part, far_part))
        return pl.multiple_of(device * rows + part * piece, piece)

    def project(group):
        tokens = [token(group, s) for s in range(4)]
        lane = lax.broadcasted_iota(jnp.int32, (piece, HEAD), 1)

        def columns(n, _):
            both = _dot(xs[group], w[n], 1, 0).astype(jnp.bfloat16)
            for s in range(4):
                t = trig[pl.ds(tokens[s], piece), :]
                swapped = pltpu.roll(t, HEAD // 2, 1)
                cos = jnp.where(lane < HEAD // 2, t, swapped)
                sin = jnp.where(lane < HEAD // 2, -swapped, t)
                for h in range(WIDE // HEAD):
                    a = both[s * piece : (s + 1) * piece, h * HEAD : (h + 1) * HEAD].astype(jnp.float32)
                    qk_ref[n * (WIDE // HEAD) + h, pl.ds(tokens[s], piece), :] = (a * cos + pltpu.roll(a, HEAD // 2, 1) * sin).astype(
                        jnp.bfloat16
                    )

        lax.fori_loop(0, heads * HEAD // WIDE, columns, None)
        v = _dot(xs[group], w_last[...], 1, 0).astype(jnp.bfloat16)
        for s in range(4):
            v_ref[pl.ds(tokens[s], piece), :] = v[s * piece : (s + 1) * piece]

    def turn(i, _):
        @pl.when(i == 1)
        def _():
            for p in range(4):
                _send(at(1 - core, p), at(1 - core, p), own_s.at[p], own_r.at[p], partner).wait_recv()

        @pl.when(i >= 2)
        def _():
            k = i - 2
            go_right(k, at(2 + k, core)).wait_recv()
            over(k, 0).start()

            @pl.when(k < 2)
            def _():
                go_right(4 + k, at(2 + k, core)).start()

            go_left(k, at(2 + k, 2 + core)).wait_recv()
            over(k, 1).start()

            @pl.when(k < 2)
            def _():
                go_left(4 + k, at(2 + k, 2 + core)).start()

            over(k, 0).wait_recv()
            over(k, 1).wait_recv()

        project(jnp.where(i == 0, core, jnp.where(i == 1, 1 - core, i)))

    lax.fori_loop(0, 8, turn, None)

    def finish(k, _):
        go_right(k, at(core, 0)).wait_send()
        go_left(k, at(core, 0)).wait_send()
        over(k, 0).wait_send()
        over(k, 1).wait_send()

    lax.fori_loop(0, 6, finish, None)
    for p in range(4):
        over_own(p).wait_send()


def _scatter(qk_ref, v_ref, wo_ref, x_ref, y_ref, wo, seen, qs, vt, mix, top, own, give, buf, through_left, through_right, end_left,
             end_right, total, xr, wo_sem, x_sem, y_sem, give_s, give_r, ring_s, through_left_r, through_right_r, end_left_r, end_right_r):
    chip, core, right, left, partner = _places()
    ready = _greet((right, left, partner))
    half = seen.shape[0] // 2
    heads = qs.shape[0]
    tiles = wo.shape[0]
    mid = tiles // 2
    rows = 2 * half
    e = HEAD**-0.5 * LOG2E

    fetches = [pltpu.make_async_copy(wo_ref.at[:, t * TILE : (t + 1) * TILE], wo.at[t], wo_sem.at[t]) for t in range(tiles)]
    for f in fetches:
        f.start()
    x_load = pltpu.make_async_copy(x_ref, xr, x_sem)
    x_load.start()

    vt[: HEAD, :] = v_ref[...].T
    vt[HEAD:, :] = jnp.ones((vt.shape[0] - HEAD, vt.shape[1]), vt.dtype)

    def where(s):
        edge = (s < 2) | (s >= 6)
        d = jnp.where(s < 2, 2, jnp.where(s >= 6, 0, jnp.where(lax.rem(s, 2) == 0, 1, 3)))
        return d, jnp.where(edge, lax.rem(s, 2), (s - 2) // 2)

    def attend(s):
        d, r = where(s)
        to = lax.rem(chip + d, CHIPS)
        starts = [pl.multiple_of((to * CORES + c) * rows + r * half, half) for c in (1 - core, core)]
        for h in range(heads):
            for i, a in enumerate(starts):
                qs[h, i * half : (i + 1) * half, :] = qk_ref[h, pl.ds(a, half), :]
        top[...] = jnp.full(top.shape, NEG, jnp.float32)
        mix[...] = jnp.zeros(mix.shape, jnp.float32)

        def block(j, masked):
            here = pl.ds(pl.multiple_of(j * KEYS, KEYS), KEYS)
            k = qk_ref[heads, here, :]
            values = vt[:, here]
            scores = [_dot(k, qs[h], 1, 1) for h in range(heads)]
            if masked:
                lane = lax.broadcasted_iota(jnp.int32, (KEYS, rows), 1)
                query = lane + jnp.where(lane < half, starts[0], starts[1] - half)
                ok = query >= lax.broadcasted_iota(jnp.int32, (KEYS, rows), 0) + j * KEYS
            weights, keeps = [], []
            for h, sc in enumerate(scores):
                if masked:
                    sc = jnp.where(ok, sc, HIDDEN)
                old = top[h : h + 1, :]
                new = jnp.maximum(old, sc.max(axis=0, keepdims=True))
                top[h : h + 1, :] = new
                weights.append(jnp.exp2((sc - new) * e).astype(jnp.bfloat16))
                keeps.append(jnp.exp2((old - new) * e))
            for h, (p, keep) in enumerate(zip(weights, keeps)):
                mix[h] = mix[h] * keep + _dot(values, p, 1, 0)

        lax.fori_loop(0, to * (CORES * rows // KEYS), lambda j, _: block(j, False), None)
        lax.fori_loop(to * (CORES * rows // KEYS), (to + 1) * (CORES * rows // KEYS), lambda j, _: block(j, True), None)
        for h in range(heads):
            seen[:, h * HEAD : (h + 1) * HEAD] = (mix[h, :HEAD, :] * (1 / mix[h, HEAD : HEAD + 1, :])).T.astype(jnp.bfloat16)

    def give_copy(s, t):
        return _send(give.at[t], buf.at[s, t], give_s.at[t], give_r.at[s, t], partner)

    def ring(s, t, dst, sem, device):
        return _send(buf.at[s, t], dst, ring_s.at[s, t], sem, device)

    def step(s, _):
        attend(s)
        d, r = where(s)

        @pl.when(s == 0)
        def _():
            for f in fetches:
                f.wait()
            ready()

        def order(j):
            far = lax.rem(j, 2) * mid + j // 2
            return jnp.where(s < 2, far, jnp.where(d == 1, lax.rem(j + mid, tiles), j))

        def turn(j, _):
            @pl.when(j < tiles)
            def _():
                t = order(j)
                both = _dot(seen[...], wo[t], 1, 0)
                own[lax.rem(j, SLOTS)] = both[half:]

                @pl.when(s > 0)
                def _():
                    give_copy(s, t).wait_send()

                give[t] = both[:half].astype(jnp.bfloat16)
                give_copy(s, t).start()

            @pl.when(j >= LAG)
            def _():
                i = j - LAG
                t = order(i)
                give_copy(s, t).wait_recv()
                mine = own.at[lax.rem(i, SLOTS)]
                added = mine[...] + buf[s, t].astype(jnp.float32)

                @pl.when(d == 0)
                def _():
                    total[r, t] = added

                @pl.when(d != 0)
                def _():
                    from_left = (d == 1) & (t < mid)
                    from_right = (d == 3) & (t >= mid)

                    @pl.when(from_left)
                    def _():
                        got = through_left.at[r, t]
                        _send(got, got, ring_s.at[s, t], through_left_r.at[r, t], right).wait_recv()
                        buf[s, t] = (added + got[...].astype(jnp.float32)).astype(jnp.bfloat16)

                    @pl.when(from_right)
                    def _():
                        got = through_right.at[r, t - mid]
                        _send(got, got, ring_s.at[s, t], through_right_r.at[r, t - mid], left).wait_recv()
                        buf[s, t] = (added + got[...].astype(jnp.float32)).astype(jnp.bfloat16)

                    @pl.when(jnp.logical_not(from_left | from_right))
                    def _():
                        buf[s, t] = added.astype(jnp.bfloat16)

                    @pl.when(d == 1)
                    def _():
                        ring(s, t, end_left.at[r, t], end_left_r.at[r, t], right).start()

                    @pl.when(d == 3)
                    def _():
                        ring(s, t, end_right.at[r, t], end_right_r.at[r, t], left).start()

                    @pl.when((d == 2) & (t < mid))
                    def _():
                        ring(s, t, through_left.at[r, t], through_left_r.at[r, t], right).start()

                    @pl.when((d == 2) & (t >= mid))
                    def _():
                        ring(s, t, through_right.at[r, t - mid], through_right_r.at[r, t - mid], left).start()

        lax.fori_loop(0, tiles + LAG, turn, None)

    lax.fori_loop(0, 8, step, None)
    x_load.wait()

    def y_copy(r, t):
        here = (pl.ds(pl.multiple_of(r * half, half), half), pl.ds(pl.multiple_of(t * TILE, TILE), TILE))
        return pltpu.make_async_copy(xr.at[here], y_ref.at[here], y_sem.at[r, t])

    def end(i, _):
        r, t = i // tiles, lax.rem(i, tiles)
        a, b = end_left.at[r, t], end_right.at[r, t]
        _send(a, a, ring_s.at[0, 0], end_left_r.at[r, t], right).wait_recv()
        _send(b, b, ring_s.at[0, 0], end_right_r.at[r, t], left).wait_recv()
        here = (pl.ds(pl.multiple_of(r * half, half), half), pl.ds(pl.multiple_of(t * TILE, TILE), TILE))
        summed = total[r, t] + a[...].astype(jnp.float32) + b[...].astype(jnp.float32)
        xr[here] = (xr[here].astype(jnp.float32) + summed).astype(jnp.bfloat16)
        y_copy(r, t).start()

    lax.fori_loop(0, 2 * tiles, end, None)

    def finish(t, _):
        give_copy(0, t).wait_send()
        for s in range(6):
            ring(s, t, buf.at[s, t], ring_s.at[s, t], right).wait_send()
        for r in range(2):
            y_copy(r, t).wait()

    lax.fori_loop(0, tiles, finish, None)


def _turns(rows):
    half = HEAD // 2
    freq = np.float32(THETA) ** (-np.arange(half, dtype=np.float32) / np.float32(half))
    angle = (np.arange(rows, dtype=np.float32)[:, None] * freq).astype(np.float64)
    return np.concatenate([np.cos(angle), np.sin(angle)], 1).astype(np.float32)


def solution(mesh):
    def step(x, gain, wq, wk, wv, wo):
        rows, d = x.shape
        n = mesh.shape["tp"]
        tokens = n * rows
        heads = wq.shape[1] // HEAD
        half, tiles = rows // 2, d // TILE
        bf16, f32 = jnp.bfloat16, jnp.float32
        any_, vmem, dma = pl.BlockSpec(memory_space=pl.ANY), pl.BlockSpec(memory_space=pltpu.VMEM), pltpu.SemaphoreType.DMA
        qk, v = pl.pallas_call(
            _gather,
            out_shape=[jax.ShapeDtypeStruct((heads + 1, tokens, HEAD), bf16), jax.ShapeDtypeStruct((tokens, HEAD), bf16)],
            in_specs=[any_, vmem, any_, any_, any_, any_],
            out_specs=[vmem, vmem],
            scratch_shapes=[
                pltpu.VMEM((n, rows, d), bf16),
                pltpu.VMEM(((heads + 1) * HEAD // WIDE, d, WIDE), bf16),
                pltpu.VMEM((d, HEAD), bf16),
                pltpu.VMEM((tokens, HEAD), f32),
                dma((4,)), dma((8,)), dma((6,)), dma((6,)), dma((6,)), dma((6,)), dma((4,)), dma((4,)), dma((2, 6)), dma((2, 6)),
            ],
            compiler_params=pltpu.CompilerParams(collective_id=0, has_side_effects=True, vmem_limit_bytes=VMEM),
            name="gather",
        )(x, gain.reshape(1, d), jnp.asarray(_turns(tokens)), wq, wk, wv)
        return pl.pallas_call(
            _scatter,
            out_shape=jax.ShapeDtypeStruct((rows, d), bf16),
            in_specs=[vmem, vmem, any_, any_],
            out_specs=any_,
            scratch_shapes=[
                pltpu.VMEM((tiles, heads * HEAD, TILE), bf16),
                pltpu.VMEM((rows, heads * HEAD), bf16),
                pltpu.VMEM((heads, rows, HEAD), bf16),
                pltpu.VMEM((HEAD + 16, tokens), bf16),
                pltpu.VMEM((heads, HEAD + 16, rows), f32),
                pltpu.VMEM((8, rows), f32),
                pltpu.VMEM((SLOTS, half, TILE), f32),
                pltpu.VMEM((tiles, half, TILE), bf16),
                pltpu.VMEM((8, tiles, half, TILE), bf16),
                pltpu.VMEM((2, tiles // 2, half, TILE), bf16),
                pltpu.VMEM((2, tiles // 2, half, TILE), bf16),
                pltpu.VMEM((2, tiles, half, TILE), bf16),
                pltpu.VMEM((2, tiles, half, TILE), bf16),
                pltpu.VMEM((2, tiles, half, TILE), f32),
                pltpu.VMEM((rows, d), bf16),
                dma((tiles,)), dma, dma((2, tiles)), dma((tiles,)), dma((8, tiles)), dma((6, tiles)),
                dma((2, tiles // 2)), dma((2, tiles // 2)), dma((2, tiles)), dma((2, tiles)),
            ],
            compiler_params=pltpu.CompilerParams(collective_id=1, has_side_effects=True, vmem_limit_bytes=VMEM),
            name="scatter",
        )(qk, v, wo, x)

    tokens, columns = P(("dp", "tp"), None), P(None, "tp")
    return jax.shard_map(
        step,
        mesh=mesh,
        in_specs=(tokens, P(None), columns, columns, columns, P("tp", None)),
        out_specs=tokens,
        check_vma=False,
    )
```

```python
import functools

import jax
import jax.numpy as jnp
import numpy as np
from jax import lax
from jax.experimental import pallas as pl
from jax.experimental.pallas import tpu as pltpu
from jax.sharding import PartitionSpec as P

HEAD = 128
THETA = 10000
NEG = -1e30
HIDDEN = 2 * NEG
LOG2E = 1.4426950408889634
VMEM = 67043328
CORES = 2
CHIPS = 4
WIDE = 256
TILE = 512
KEYS = 512
LAG = 4
SLOTS = 5


def _dot(a, b, ca, cb):
    return lax.dot_general(a, b, (((ca,), (cb,)), ((), ())), preferred_element_type=jnp.float32)


def _places():
    me = lax.axis_index("tp")
    chip, core = me // CORES, lax.rem(me, CORES)
    right = lax.rem(chip + 1, CHIPS) * CORES + core
    left = lax.rem(chip + CHIPS - 1, CHIPS) * CORES + core
    return chip, core, right, left, chip * CORES + 1 - core


def _greet(peers):
    barrier = pltpu.get_barrier_semaphore()
    for peer in peers:
        pl.semaphore_signal(barrier, inc=1, device_id={"tp": peer}, device_id_type=pl.DeviceIdType.MESH)
    return lambda: pl.semaphore_wait(barrier, len(peers))


def _send(src, dst, send_sem, recv_sem, device):
    return pltpu.make_async_remote_copy(src_ref=src, dst_ref=dst, send_sem=send_sem, recv_sem=recv_sem, device_id={"tp": device},
                                        device_id_type=pl.DeviceIdType.MESH)


def _attention(x_ref, gain_ref, trig_ref, wq_ref, wk_ref, wv_ref, wo_ref, y_ref, xs, w, w_last, trig, qk, v, vt, qs, seen, mix, top, own, give,
               xr, x_sem, w_sem, wo_sem, xr_sem, y_sem, right_s, right_r, left_s, left_r, own_s, own_r, pass_s, pass_r, free_early,
               free_late, give_s, give_r, ring_s, through_left_r, through_right_r, end_left_r, end_right_r):
    chip, core, right, left, partner = _places()
    peers = (right, left, partner)
    ready = _greet(peers)
    rows, d = x_ref.shape
    piece, half = rows // 4, rows // 2
    heads = qs.shape[0]
    tiles = d // TILE
    mid = tiles // 2
    fold = TILE // 2
    e = HEAD**-0.5 * LOG2E

    def at(group, slot):
        return xs.at[pl.ds(pl.multiple_of(group * rows + slot * piece, piece), piece)]

    loads = [pltpu.make_async_copy(x_ref.at[pl.ds(p * piece, piece)], at(core, p), x_sem.at[p]) for p in range(4)]
    for p in (0, 2, 1, 3):
        loads[p].start()
    n_q = wq_ref.shape[1]
    n_last = n_q // WIDE
    blocks = [(wq_ref.at[:, n * WIDE : (n + 1) * WIDE], w.at[n]) for n in range(n_last)]
    blocks.append((wq_ref.at[:, n_last * WIDE :], w.at[n_last, :, : WIDE - HEAD]))
    blocks.append((wk_ref, w.at[n_last, :, WIDE - HEAD :]))
    blocks.append((wv_ref, w_last))
    blocks.append((trig_ref, trig))
    fetches = [pltpu.make_async_copy(a, b, w_sem.at[n]) for n, (a, b) in enumerate(blocks)]
    for f in fetches:
        f.start()

    gain = gain_ref[...].reshape(1, d).astype(jnp.float32)

    def norm(p):
        def body(i, _):
            here = pl.ds(pl.multiple_of(core * rows + p * piece + i * 16, 16), 16)
            wide = xs[here, :].astype(jnp.float32)
            scale = lax.rsqrt(jnp.mean(wide * wide, -1, keepdims=True) + 1e-6)
            xs[here, :] = (wide * scale * gain).astype(jnp.bfloat16)

        lax.fori_loop(0, piece // 16, body, None)

    def go_right(k, src):
        return _send(src, at(2 + k, 2 * core), right_s.at[k], right_r.at[k], right)

    def go_left(k, src):
        return _send(src, at(2 + k, 2 * core + 1), left_s.at[k], left_r.at[k], left)

    def over_own(p):
        return _send(at(core, p), at(core, p), own_s.at[p], own_r.at[p], partner)

    def over(k, side):
        here = at(2 + k, 2 * core + side)
        return _send(here, here, pass_s.at[side, k], pass_r.at[side, k], partner)

    def own_right(k):
        return go_right(k, at(core, k))

    def own_left(k):
        return go_left(k, at(core, (k + 2) % 4))

    for i, p in enumerate((0, 2, 1, 3)):
        loads[p].wait()
        norm(p)
        if i == 0:
            ready()
        if p < 2:
            own_right(p).start()
        else:
            own_left(p - 2).start()
        over_own(p).start()
    for k in (2, 3):
        own_right(k).start()
        own_left(k).start()
    x_load = pltpu.make_async_copy(x_ref, xr, xr_sem)
    x_load.start()
    for f in fetches:
        f.wait()

    def place(group, slot):
        k = group - 2
        c, side = slot // 2, slot % 2
        near = lax.rem(chip + (1 if side else CHIPS - 1), CHIPS)
        near_part = lax.rem(k + 2, 4) if side else k
        far_part = k - 4 + 2 * side
        to = jnp.where(group < 2, chip, jnp.where(group < 6, near, lax.rem(chip + 2, CHIPS)))
        c = jnp.where(group < 2, group, c)
        part = jnp.where(group < 2, slot, jnp.where(group < 6, near_part, far_part))
        return pl.multiple_of(to * CORES * rows + lax.rem(part, 2) * rows + c * half + part // 2 * piece, piece)

    def project(group, first, last, values):
        places = [place(group, s) for s in range(4)]
        lane = lax.broadcasted_iota(jnp.int32, (piece, HEAD), 1)
        a_ref = xs.at[pl.ds(pl.multiple_of(group * rows, rows), rows)]

        def columns(n, _):
            both = _dot(a_ref[...], w[n], 1, 0).astype(jnp.bfloat16)
            for s in range(4):
                t = trig[pl.ds(places[s], piece), :]
                swapped = pltpu.roll(t, HEAD // 2, 1)
                cos = jnp.where(lane < HEAD // 2, t, swapped)
                sin = jnp.where(lane < HEAD // 2, -swapped, t)
                for h in range(WIDE // HEAD):
                    a = both[s * piece : (s + 1) * piece, h * HEAD : (h + 1) * HEAD].astype(jnp.float32)
                    qk[n * (WIDE // HEAD) + h, pl.ds(places[s], piece), :] = (a * cos + pltpu.roll(a, HEAD // 2, 1) * sin).astype(
                        jnp.bfloat16
                    )

        lax.fori_loop(first, last, columns, None)
        if values:
            both = _dot(a_ref[...], w_last[...], 1, 0).astype(jnp.bfloat16)
            for s in range(4):
                v[pl.ds(places[s], piece), :] = both[s * piece : (s + 1) * piece]

    def arrive(k):
        go_right(k, at(2 + k, 2 * core)).wait_recv()
        over(k, 0).start()

        @pl.when(k < 2)
        def _():
            go_right(4 + k, at(2 + k, 2 * core)).start()

        go_left(k, at(2 + k, 2 * core + 1)).wait_recv()
        over(k, 1).start()

        @pl.when(k < 2)
        def _():
            go_left(4 + k, at(2 + k, 2 * core + 1)).start()

    def turn(i, _):
        @pl.when(i == 1)
        def _():
            for p in range(4):
                _send(at(1 - core, p), at(1 - core, p), own_s.at[p], own_r.at[p], partner).wait_recv()

        @pl.when(i >= 2)
        def _():
            arrive(i - 2)
            over(i - 2, 0).wait_recv()
            over(i - 2, 1).wait_recv()

        project(jnp.where(i == 0, core, jnp.where(i == 1, 1 - core, i)), 0, n_last + 1, True)

    lax.fori_loop(0, 7, turn, None)

    def stage(s):
        edge = (s < 2) | (s >= 6)
        dist = jnp.where(s < 2, 2, jnp.where(s >= 6, 0, jnp.where(lax.rem(s, 2) == 0, 1, 3)))
        return dist, jnp.where(edge, lax.rem(s, 2), (s - 2) // 2)

    def block(start, keys, level):
        here = pl.ds(pl.multiple_of(start, keys), keys)
        k = qk[heads, here, :]
        values = vt[:, here]
        scores = [_dot(k, qs[h], 1, 1) for h in range(heads)]
        if level is not None:
            row = lax.broadcasted_iota(jnp.int32, (keys, rows), 0)
            lane = lax.broadcasted_iota(jnp.int32, (keys, rows), 1)
            key = row + (row // piece) * piece
            query_core = jnp.where(lane < half, 1 - core, core)
            inner = lax.rem(lane, half)
            query = query_core * rows + inner + (inner // piece) * piece
            ok = query + level * piece >= key
        weights, keeps = [], []
        for h, sc in enumerate(scores):
            if level is not None:
                sc = jnp.where(ok, sc, HIDDEN)
            old = top[h : h + 1, :]
            new = jnp.maximum(old, sc.max(axis=0, keepdims=True))
            top[h : h + 1, :] = new
            weights.append(jnp.exp2((sc - new) * e).astype(jnp.bfloat16))
            keeps.append(jnp.exp2((old - new) * e))
        for h, (p, keep) in enumerate(zip(weights, keeps)):
            mix[h] = mix[h] * keep + _dot(values, p, 1, 0)

    def attend_first(s):
        dist, r = stage(s)
        base = lax.rem(chip + dist, CHIPS) * (CORES * rows)
        for h in range(heads):
            for i, c in enumerate((1 - core, core)):
                qs[h, i * half : (i + 1) * half, :] = qk[h, pl.ds(pl.multiple_of(base + r * rows + c * half, half), half), :]
        top[...] = jnp.full(top.shape, NEG, jnp.float32)
        mix[...] = jnp.zeros(mix.shape, jnp.float32)
        lax.fori_loop(0, base // KEYS, lambda j, _: block(j * KEYS, KEYS, None), None)
        block(base, rows, r)

    def attend_last(s):
        dist, r = stage(s)
        base = lax.rem(chip + dist, CHIPS) * (CORES * rows)
        block(base + rows, rows, r - 1)
        for h in range(heads):
            seen[:, h * HEAD : (h + 1) * HEAD] = (mix[h, :HEAD, :] * (1 / mix[h, HEAD : HEAD + 1, :])).T.astype(jnp.bfloat16)

    def turn_values(j):
        here = pl.ds(pl.multiple_of(j * rows, rows), rows)
        vt[:HEAD, here] = v[here, :].T

    last = lax.rem(chip + 2, CHIPS) * CORES + 1
    vt[HEAD:, :] = jnp.ones((vt.shape[0] - HEAD, vt.shape[1]), vt.dtype)
    lax.fori_loop(1, CHIPS * CORES, lambda j, _: turn_values(lax.rem(last + j, CHIPS * CORES)), None)

    for k in (2, 3):
        over(k, 0).wait_send()
        over(k, 1).wait_send()
    for peer in peers:
        pl.semaphore_signal(free_early, inc=1, device_id={"tp": peer}, device_id_type=pl.DeviceIdType.MESH)
    attend_first(0)

    arrive(5)
    for k in range(6):
        go_right(k, at(core, 0)).wait_send()
        go_left(k, at(core, 0)).wait_send()
    for p in range(4):
        over_own(p).wait_send()
    for k in (0, 1):
        over(k, 0).wait_send()
        over(k, 1).wait_send()
    depth = wo_ref.shape[0]
    wo_loads = []
    for n in range(2):
        here = pl.ds(n * mid * TILE, mid * TILE)
        wo_loads.append(pltpu.make_async_copy(wo_ref.at[:, here], xs.at[pl.ds(0, depth), here], wo_sem.at[n]))
        wo_loads[n].start()
    over(5, 0).wait_recv()
    over(5, 1).wait_recv()
    project(7, n_last, n_last + 1, True)
    turn_values(last)

    def tile(group, n):
        return xs.at[pl.ds(pl.multiple_of(group * rows, rows), rows), pl.ds(pl.multiple_of(n * fold, fold), fold)]

    def ring_tile(s, t):
        n = jnp.maximum(s - 2, 0) * tiles + t
        per = w.shape[1] // rows
        return tile(5, jnp.minimum(s, 1) * tiles + t), w.at[1 + n // per, pl.ds(pl.multiple_of(lax.rem(n, per) * rows, rows), rows), :]

    def folded(a):
        return jnp.concatenate([a[:, :fold], a[:, fold:]], axis=0)

    def give_copy(t, dst, sem):
        return _send(give.at[t], dst, give_s.at[t], sem, partner)

    def step(s, _):
        dist, r = stage(s)

        @pl.when(s > 0)
        def _():
            attend_first(s)

        attend_last(s)

        @pl.when(s == 0)
        def _():
            for f in wo_loads:
                f.wait()
            pl.semaphore_wait(free_early, len(peers))

        @pl.when(s == 2)
        def _():
            pl.semaphore_wait(free_late, len(peers))

        def order(j):
            both = lax.rem(j, 2) * mid + j // 2
            return jnp.where(dist == 1, lax.rem(j + mid, tiles), jnp.where(dist == 3, j, both))

        def turn(j, _):
            @pl.when(j < tiles)
            def _():
                t = order(j)
                both = _dot(seen[...], xs[pl.ds(0, depth), pl.ds(pl.multiple_of(t * TILE, TILE), TILE)], 1, 0)
                own[lax.rem(j, SLOTS)] = folded(both[half:])

                @pl.when(s > 0)
                def _():
                    give_copy(t, give.at[t], give_r.at[s, t]).wait_send()

                give[t] = folded(both[:half].astype(jnp.bfloat16))
                early, late = ring_tile(s, t)

                @pl.when(s < 2)
                def _():
                    give_copy(t, early, give_r.at[s, t]).start()

                @pl.when(s >= 2)
                def _():
                    give_copy(t, late, give_r.at[s, t]).start()

            @pl.when(j >= LAG)
            def _():
                i = j - LAG
                t = order(i)
                give_copy(t, give.at[t], give_r.at[s, t]).wait_recv()
                mine = own.at[lax.rem(i, SLOTS)]
                early, late = ring_tile(s, t)

                @pl.when(s < 2)
                def _():
                    early[...] = (mine[...] + early[...].astype(jnp.float32)).astype(jnp.bfloat16)

                    @pl.when(t < mid)
                    def _():
                        _send(early, tile(4, r * tiles + t), ring_s.at[s, t], through_left_r.at[r, t], right).start()

                    @pl.when(t >= mid)
                    def _():
                        _send(early, tile(4, r * tiles + t), ring_s.at[s, t], through_right_r.at[r, t - mid], left).start()

                from_left = (dist == 1) & (t < mid)
                from_right = (dist == 3) & (t >= mid)
                got = tile(4, r * tiles + t)

                @pl.when(from_left)
                def _():
                    _send(got, got, give_s.at[t], through_left_r.at[r, t], right).wait_recv()

                @pl.when(from_right)
                def _():
                    _send(got, got, give_s.at[t], through_right_r.at[r, t - mid], left).wait_recv()

                @pl.when(from_left | from_right)
                def _():
                    late[...] = (mine[...] + late[...].astype(jnp.float32) + got[...].astype(jnp.float32)).astype(jnp.bfloat16)

                @pl.when((s >= 2) & (s < 6) & jnp.logical_not(from_left | from_right))
                def _():
                    late[...] = (mine[...] + late[...].astype(jnp.float32)).astype(jnp.bfloat16)

                @pl.when(dist == 1)
                def _():
                    _send(late, tile(6, r * tiles + t), ring_s.at[s, t], end_left_r.at[r, t], right).start()

                @pl.when(dist == 3)
                def _():
                    _send(late, tile(7, r * tiles + t), ring_s.at[s, t], end_right_r.at[r, t], left).start()

                @pl.when(dist == 0)
                def _():
                    a, b = tile(6, r * tiles + t), tile(7, r * tiles + t)
                    _send(a, a, give_s.at[t], end_left_r.at[r, t], right).wait_recv()
                    _send(b, b, give_s.at[t], end_right_r.at[r, t], left).wait_recv()
                    summed = mine[...] + late[...].astype(jnp.float32) + a[...].astype(jnp.float32) + b[...].astype(jnp.float32)
                    for u in range(half // piece):
                        for side in range(2):
                            here = (pl.ds(pl.multiple_of((2 * u + r) * piece, piece), piece),
                                    pl.ds(pl.multiple_of(t * TILE + side * fold, fold), fold))
                            part = summed[side * half + u * piece : side * half + (u + 1) * piece]
                            xr[here] = (xr[here].astype(jnp.float32) + part).astype(jnp.bfloat16)
                        y_copy(r, t, u).start()

        lax.fori_loop(0, tiles + LAG, turn, None)

        @pl.when(s == 0)
        def _():
            project(7, 0, n_last, False)
            for k in (4, 5):
                over(k, 0).wait_send()
                over(k, 1).wait_send()
            for peer in peers:
                pl.semaphore_signal(free_late, inc=1, device_id={"tp": peer}, device_id_type=pl.DeviceIdType.MESH)
            x_load.wait()

    def y_copy(r, t, u):
        here = (pl.ds(pl.multiple_of((2 * u + r) * piece, piece), piece), pl.ds(pl.multiple_of(t * TILE, TILE), TILE))
        return pltpu.make_async_copy(xr.at[here], y_ref.at[here], y_sem.at[r, t, u])

    lax.fori_loop(0, 8, step, None)

    def finish(t, _):
        give_copy(t, give.at[t], give_r.at[0, t]).wait_send()
        for s in range(6):
            _send(give.at[t], give.at[t], ring_s.at[s, t], give_r.at[0, t], right).wait_send()
        for r in range(2):
            for u in range(2):
                y_copy(r, t, u).wait()

    lax.fori_loop(0, tiles, finish, None)


def _turns(chip_rows, chips):
    half, piece = HEAD // 2, chip_rows // 8
    freq = np.float32(THETA) ** (-np.arange(half, dtype=np.float32) / np.float32(half))
    place = np.arange(chip_rows * chips).reshape(chips, CORES, 2, 2, piece).transpose(0, 3, 1, 2, 4).reshape(-1)
    angle = (place.astype(np.float32)[:, None] * freq).astype(np.float64)
    return np.concatenate([np.cos(angle), np.sin(angle)], 1).astype(np.float32)


def solution(mesh):
    def step(x, gain, wq, wk, wv, wo):
        rows, d = x.shape
        n = mesh.shape["tp"]
        tokens = n * rows
        heads = wq.shape[1] // HEAD
        half, tiles = rows // 2, d // TILE
        bf16, f32 = jnp.bfloat16, jnp.float32
        any_, vmem, dma = pl.BlockSpec(memory_space=pl.ANY), pl.BlockSpec(memory_space=pltpu.VMEM), pltpu.SemaphoreType.DMA
        regular = pltpu.SemaphoreType.REGULAR
        return pl.pallas_call(
            _attention,
            out_shape=jax.ShapeDtypeStruct((rows, d), bf16),
            in_specs=[any_, vmem, any_, any_, any_, any_, any_],
            out_specs=any_,
            scratch_shapes=[
                pltpu.VMEM((n * rows, d), bf16),
                pltpu.VMEM(((heads + 1) * HEAD // WIDE, d, WIDE), bf16),
                pltpu.VMEM((d, HEAD), bf16),
                pltpu.VMEM((tokens, HEAD), f32),
                pltpu.VMEM((heads + 1, tokens, HEAD), bf16),
                pltpu.VMEM((tokens, HEAD), bf16),
                pltpu.VMEM((HEAD + 16, tokens), bf16),
                pltpu.VMEM((heads, rows, HEAD), bf16),
                pltpu.VMEM((rows, heads * HEAD), bf16),
                pltpu.VMEM((heads, HEAD + 16, rows), f32),
                pltpu.VMEM((8, rows), f32),
                pltpu.VMEM((SLOTS, rows, TILE // 2), f32),
                pltpu.VMEM((tiles, rows, TILE // 2), bf16),
                pltpu.VMEM((rows, d), bf16),
                dma((4,)), dma((8,)), dma((2,)), dma, dma((2, tiles, 2)),
                dma((6,)), dma((6,)), dma((6,)), dma((6,)), dma((4,)), dma((4,)), dma((2, 6)), dma((2, 6)),
                regular, regular,
                dma((tiles,)), dma((8, tiles)), dma((6, tiles)),
                dma((2, tiles // 2)), dma((2, tiles // 2)), dma((2, tiles)), dma((2, tiles)),
            ],
            compiler_params=pltpu.CompilerParams(collective_id=0, has_side_effects=True, vmem_limit_bytes=VMEM),
            name="attention",
        )(x, gain, jnp.asarray(_turns(CORES * rows, n // CORES)), wq, wk, wv, wo)

    tokens, columns = P(("dp", "tp"), None), P(None, "tp")
    return jax.shard_map(
        step,
        mesh=mesh,
        in_specs=(tokens, P(None), columns, columns, columns, P("tp", None)),
        out_specs=tokens,
        check_vma=False,
    )
```

```python
import functools

import jax
import jax.numpy as jnp
import numpy as np
from jax import lax
from jax.experimental import pallas as pl
from jax.experimental.pallas import tpu as pltpu
from jax.sharding import PartitionSpec as P

HEAD = 128
THETA = 10000
NEG = -1e30
HIDDEN = 2 * NEG
LOG2E = 1.4426950408889634
VMEM = 67043328
CORES = 2
CHIPS = 4
WIDE = 256
TILE = 512
KEYS = 512
LAG = 2
SLOTS = 3
GIVES = 4


def _dot(a, b, ca, cb):
    return lax.dot_general(a, b, (((ca,), (cb,)), ((), ())), preferred_element_type=jnp.float32)


def _places():
    me = lax.axis_index("tp")
    chip, core = me // CORES, lax.rem(me, CORES)
    right = lax.rem(chip + 1, CHIPS) * CORES + core
    left = lax.rem(chip + CHIPS - 1, CHIPS) * CORES + core
    return chip, core, right, left, chip * CORES + 1 - core


def _greet(peers):
    barrier = pltpu.get_barrier_semaphore()
    for peer in peers:
        pl.semaphore_signal(barrier, inc=1, device_id={"tp": peer}, device_id_type=pl.DeviceIdType.MESH)
    return lambda: pl.semaphore_wait(barrier, len(peers))


def _send(src, dst, send_sem, recv_sem, device):
    return pltpu.make_async_remote_copy(src_ref=src, dst_ref=dst, send_sem=send_sem, recv_sem=recv_sem, device_id={"tp": device},
                                        device_id_type=pl.DeviceIdType.MESH)


def _attention(x_ref, gain_ref, trig_ref, wq_ref, wk_ref, wv_ref, wo_ref, y_ref, xs, w, w_last, trig, qk, v, vt, qs, seen, mix, top, own, give,
               xr, x_sem, w_sem, wo_sem, xr_sem, y_sem, right_s, right_r, left_s, left_r, own_s, own_r, pass_s, pass_r, free_early,
               free_late, give_s, give_r, ring_s, through_left_r, through_right_r, end_left_r, end_right_r):
    chip, core, right, left, partner = _places()
    peers = (right, left, partner)
    ready = _greet(peers)
    rows, d = x_ref.shape
    piece, half = rows // 4, rows // 2
    heads = qs.shape[0]
    tiles = d // TILE
    mid = tiles // 2
    fold = TILE // 2
    e = HEAD**-0.5 * LOG2E

    stripe = piece // 2

    def at(group, slot, b):
        return xs.at[pl.ds(pl.multiple_of(group * rows + slot * piece + b * stripe, stripe), stripe)]

    in_turn = [(p, b) for p in (0, 1) for b in range(2)]
    in_turn = [(p + 2 * side, b) for p, b in in_turn for side in range(2)]
    loads = {
        (p, b): pltpu.make_async_copy(x_ref.at[pl.ds(p * piece + b * stripe, stripe)], at(core, p, b), x_sem.at[p, b])
        for p, b in in_turn
    }
    for f in loads.values():
        f.start()
    n_q = wq_ref.shape[1]
    n_last = n_q // WIDE
    blocks = [(wq_ref.at[:, n * WIDE : (n + 1) * WIDE], w.at[n]) for n in range(n_last)]
    blocks.append((wk_ref, w.at[n_last, :, :HEAD]))
    blocks.append((wv_ref, w.at[n_last, :, HEAD:]))
    blocks.append((wq_ref.at[:, n_last * WIDE :], w_last))
    blocks.append((trig_ref, trig))
    fetches = [pltpu.make_async_copy(a, b, w_sem.at[n]) for n, (a, b) in enumerate(blocks)]

    gain = gain_ref[...].reshape(1, d).astype(jnp.float32)

    def norm(p, b):
        def body(i, _):
            here = pl.ds(pl.multiple_of(core * rows + p * piece + b * stripe + i * 16, 16), 16)
            wide = xs[here, :].astype(jnp.float32)
            scale = lax.rsqrt(jnp.mean(wide * wide, -1, keepdims=True) + 1e-6)
            xs[here, :] = (wide * scale * gain).astype(jnp.bfloat16)

        lax.fori_loop(0, stripe // 16, body, None)

    def go_right(k, b, src):
        return _send(src, at(2 + k, 2 * core, b), right_s.at[k, b], right_r.at[k, b], right)

    def go_left(k, b, src):
        return _send(src, at(2 + k, 2 * core + 1, b), left_s.at[k, b], left_r.at[k, b], left)

    def over_own(p, b):
        return _send(at(core, p, b), at(core, p, b), own_s.at[p, b], own_r.at[p, b], partner)

    def over(k, side, b):
        here = at(2 + k, 2 * core + side, b)
        return _send(here, here, pass_s.at[side, k, b], pass_r.at[side, k, b], partner)

    def own_right(k, b):
        return go_right(k, b, at(core, k, b))

    def own_left(k, b):
        return go_left(k, b, at(core, (k + 2) % 4, b))

    for i, (p, b) in enumerate(in_turn):
        loads[p, b].wait()
        norm(p, b)
        if i == 0:
            ready()
        if p < 2:
            own_right(p, b).start()
        else:
            own_left(p - 2, b).start()
        over_own(p, b).start()
    for k in (2, 3):
        for b in range(2):
            own_right(k, b).start()
            own_left(k, b).start()
    x_load = pltpu.make_async_copy(x_ref, xr, xr_sem)
    for f in fetches:
        f.start()
    for f in fetches:
        f.wait()
    x_load.start()

    def place(group, slot):
        k = group - 2
        c, side = slot // 2, slot % 2
        near = lax.rem(chip + (1 if side else CHIPS - 1), CHIPS)
        near_part = lax.rem(k + 2, 4) if side else k
        far_part = k - 4 + 2 * side
        to = jnp.where(group < 2, chip, jnp.where(group < 6, near, lax.rem(chip + 2, CHIPS)))
        c = jnp.where(group < 2, group, c)
        part = jnp.where(group < 2, slot, jnp.where(group < 6, near_part, far_part))
        return pl.multiple_of(to * CORES * rows + lax.rem(part, 2) * rows + c * half + part // 2 * piece, piece)

    def project(group, queries, keys):
        places = [place(group, s) for s in range(4)]
        lane = lax.broadcasted_iota(jnp.int32, (piece, HEAD), 1)
        a_ref = xs.at[pl.ds(pl.multiple_of(group * rows, rows), rows)]

        def turned(both, first, count):
            for s in range(4):
                t = trig[pl.ds(places[s], piece), :]
                swapped = pltpu.roll(t, HEAD // 2, 1)
                cos = jnp.where(lane < HEAD // 2, t, swapped)
                sin = jnp.where(lane < HEAD // 2, -swapped, t)
                for h in range(count):
                    a = both[s * piece : (s + 1) * piece, h * HEAD : (h + 1) * HEAD].astype(jnp.float32)
                    qk[first + h, pl.ds(places[s], piece), :] = (a * cos + pltpu.roll(a, HEAD // 2, 1) * sin).astype(jnp.bfloat16)

        def columns(n, _):
            turned(_dot(a_ref[...], w[n], 1, 0).astype(jnp.bfloat16), n * (WIDE // HEAD), WIDE // HEAD)

        if keys:
            both = _dot(a_ref[...], w[n_last], 1, 0).astype(jnp.bfloat16)
            turned(both, heads, 1)
            for s in range(4):
                v[pl.ds(places[s], piece), :] = both[s * piece : (s + 1) * piece, HEAD:]
        if queries:
            lax.fori_loop(0, n_last, columns, None)
            turned(_dot(a_ref[...], w_last[...], 1, 0).astype(jnp.bfloat16), heads - 1, 1)

    def arrive(k):
        for b in range(2):
            go_right(k, b, at(2 + k, 2 * core, b)).wait_recv()
            over(k, 0, b).start()

            @pl.when(k < 2)
            def _():
                go_right(4 + k, b, at(2 + k, 2 * core, b)).start()

            go_left(k, b, at(2 + k, 2 * core + 1, b)).wait_recv()
            over(k, 1, b).start()

            @pl.when(k < 2)
            def _():
                go_left(4 + k, b, at(2 + k, 2 * core + 1, b)).start()

    def pass_in(k):
        for b in range(2):
            for side in range(2):
                over(k, side, b).wait_recv()

    def pass_out(k):
        for b in range(2):
            for side in range(2):
                over(k, side, b).wait_send()

    def turn(i, _):
        @pl.when(i == 1)
        def _():
            for p in range(4):
                for b in range(2):
                    here = at(1 - core, p, b)
                    _send(here, here, own_s.at[p, b], own_r.at[p, b], partner).wait_recv()

        @pl.when(i >= 2)
        def _():
            arrive(i - 2)
            pass_in(i - 2)

        project(jnp.where(i == 0, core, jnp.where(i == 1, 1 - core, i)), True, True)

    lax.fori_loop(0, 7, turn, None)

    def stage(s):
        edge = (s < 2) | (s >= 6)
        dist = jnp.where(s < 2, 2, jnp.where(s >= 6, 0, jnp.where(lax.rem(s, 2) == 0, 1, 3)))
        return dist, jnp.where(edge, lax.rem(s, 2), (s - 2) // 2)

    def block(start, keys, level):
        here = pl.ds(pl.multiple_of(start, keys), keys)
        k = qk[heads, here, :]
        values = vt[:, here]
        scores = [_dot(k, qs[h], 1, 1) for h in range(heads)]
        if level is not None:
            row = lax.broadcasted_iota(jnp.int32, (keys, rows), 0)
            lane = lax.broadcasted_iota(jnp.int32, (keys, rows), 1)
            key = row + (row // piece) * piece
            query_core = jnp.where(lane < half, 1 - core, core)
            inner = lax.rem(lane, half)
            query = query_core * rows + inner + (inner // piece) * piece
            ok = query + level * piece >= key
        weights, keeps = [], []
        for h, sc in enumerate(scores):
            if level is not None:
                sc = jnp.where(ok, sc, HIDDEN)
            old = top[h : h + 1, :]
            new = jnp.maximum(old, sc.max(axis=0, keepdims=True))
            top[h : h + 1, :] = new
            weights.append(jnp.exp2((sc - new) * e).astype(jnp.bfloat16))
            keeps.append(jnp.exp2((old - new) * e))
        for h, (p, keep) in enumerate(zip(weights, keeps)):
            mix[h] = mix[h] * keep + _dot(values, p, 1, 0)

    def attend_first(s):
        dist, r = stage(s)
        base = lax.rem(chip + dist, CHIPS) * (CORES * rows)
        for h in range(heads):
            for i, c in enumerate((1 - core, core)):
                qs[h, i * half : (i + 1) * half, :] = qk[h, pl.ds(pl.multiple_of(base + r * rows + c * half, half), half), :]
        top[...] = jnp.full(top.shape, NEG, jnp.float32)
        mix[...] = jnp.zeros(mix.shape, jnp.float32)
        lax.fori_loop(0, base // KEYS, lambda j, _: block(j * KEYS, KEYS, None), None)
        block(base, rows, r)

    def attend_last(s, seen):
        dist, r = stage(s)
        base = lax.rem(chip + dist, CHIPS) * (CORES * rows)
        block(base + rows, rows, r - 1)
        for h in range(heads):
            seen[:, h * HEAD : (h + 1) * HEAD] = (mix[h, :HEAD, :] * (1 / mix[h, HEAD : HEAD + 1, :])).T.astype(jnp.bfloat16)

    def turn_values(j):
        here = pl.ds(pl.multiple_of(j * rows, rows), rows)
        vt[:HEAD, here] = v[here, :].T

    last = lax.rem(chip + 2, CHIPS) * CORES + 1
    vt[HEAD:, :] = jnp.ones((vt.shape[0] - HEAD, vt.shape[1]), vt.dtype)
    lax.fori_loop(1, CHIPS * CORES, lambda j, _: turn_values(lax.rem(last + j, CHIPS * CORES)), None)

    for k in (2, 3):
        pass_out(k)
    for peer in peers:
        pl.semaphore_signal(free_early, inc=1, device_id={"tp": peer}, device_id_type=pl.DeviceIdType.MESH)
    attend_first(0)

    arrive(5)
    for b in range(2):
        for k in range(6):
            go_right(k, b, at(core, 0, b)).wait_send()
            go_left(k, b, at(core, 0, b)).wait_send()
        for p in range(4):
            over_own(p, b).wait_send()
    for k in (0, 1):
        pass_out(k)
    depth = wo_ref.shape[0]
    wo_loads = []
    for n in range(2):
        here = pl.ds(n * mid * TILE, mid * TILE)
        wo_loads.append(pltpu.make_async_copy(wo_ref.at[:, here], xs.at[pl.ds(0, depth), here], wo_sem.at[n]))
        wo_loads[n].start()
    pass_in(5)
    project(7, False, True)
    turn_values(last)

    def tile(group, n):
        return xs.at[pl.ds(pl.multiple_of(group * rows, rows), rows), pl.ds(pl.multiple_of(n * fold, fold), fold)]

    def ring_tile(s, t):
        n = jnp.maximum(s - 2, 0) * tiles + t
        per = w.shape[1] // rows
        return tile(5, jnp.minimum(s, 1) * tiles + t), w.at[1 + n // per, pl.ds(pl.multiple_of(lax.rem(n, per) * rows, rows), rows), :]

    def folded(a):
        return jnp.concatenate([a[:, :fold], a[:, fold:]], axis=0)

    def give_copy(slot, side, dst, sem):
        return _send(give.at[slot, side], dst, give_s.at[slot, side], sem, partner)

    pairs = tiles // 2
    some = pairs // 2

    def step(phase, _):
        again = (phase == 4) | (phase == 5)
        s = jnp.where(phase < 4, phase, phase - 2)
        dist, r = stage(s)
        first = jnp.where(again, some, 0)
        end = jnp.where((phase == 2) | (phase == 3), some, pairs)
        done = jnp.where(phase < 2, phase * pairs, jnp.where(phase < 4, 2 * pairs + (phase - 2) * some, jnp.where(
            phase < 6, 2 * pairs + 2 * some + (phase - 4) * (pairs - some), (phase - 2) * pairs)))
        lag = jnp.where(phase == 0, 1, LAG)
        mine_seen = seen.at[jnp.where((phase == 3) | (phase == 5), 1, 0)]

        @pl.when((phase > 0) & jnp.logical_not(again))
        def _():
            attend_first(s)

        @pl.when(jnp.logical_not(again))
        def _():
            attend_last(s, mine_seen)

        @pl.when(phase == 0)
        def _():
            for f in wo_loads:
                f.wait()
            pl.semaphore_wait(free_early, len(peers))

        @pl.when(phase == 2)
        def _():
            pl.semaphore_wait(free_late, len(peers))

        def order(j):
            both = lax.rem(lax.rem(j, 2) * (some + 1) + j // 2, pairs)
            return jnp.where(dist == 1, lax.rem(j + some + 1, pairs), jnp.where(dist == 3, j, both))

        def product(j):
            n = done + j - first
            pair = order(j)
            both = _dot(mine_seen[...], xs[pl.ds(0, depth), pl.ds(pl.multiple_of(pair * 2 * TILE, 2 * TILE), 2 * TILE)], 1, 0)
            slot, out = lax.rem(n, SLOTS), lax.rem(n, GIVES)

            @pl.when(n >= GIVES)
            def _():
                for b in range(2):
                    give_copy(out, b, give.at[out, b], give_r.at[s, 2 * pair + b]).wait_send()

            for b in range(2):
                t = 2 * pair + b
                give[out, b] = folded(both[:half, b * TILE : (b + 1) * TILE].astype(jnp.bfloat16))
                own[slot, b] = folded(both[half:, b * TILE : (b + 1) * TILE])
                early, late = ring_tile(s, t)

                @pl.when(s < 2)
                def _():
                    give_copy(out, b, early, give_r.at[s, t]).start()

                @pl.when(s >= 2)
                def _():
                    give_copy(out, b, late, give_r.at[s, t]).start()

        def add(j, b):
            n = done + j - first
            t = 2 * order(j) + b
            give_copy(0, b, give.at[0, b], give_r.at[s, t]).wait_recv()
            mine = own.at[lax.rem(n, SLOTS), b]
            early, late = ring_tile(s, t)

            @pl.when(s < 2)
            def _():
                early[...] = (mine[...] + early[...].astype(jnp.float32)).astype(jnp.bfloat16)

                @pl.when(t < mid)
                def _():
                    _send(early, tile(4, r * tiles + t), ring_s.at[s, t], through_left_r.at[r, t], right).start()

                @pl.when(t >= mid)
                def _():
                    _send(early, tile(4, r * tiles + t), ring_s.at[s, t], through_right_r.at[r, t - mid], left).start()

            from_left = (dist == 1) & (t < mid)
            from_right = (dist == 3) & (t >= mid)
            got = tile(4, r * tiles + t)

            @pl.when(from_left)
            def _():
                _send(got, got, give_s.at[0, b], through_left_r.at[r, t], right).wait_recv()

            @pl.when(from_right)
            def _():
                _send(got, got, give_s.at[0, b], through_right_r.at[r, t - mid], left).wait_recv()

            @pl.when(from_left | from_right)
            def _():
                late[...] = (mine[...] + late[...].astype(jnp.float32) + got[...].astype(jnp.float32)).astype(jnp.bfloat16)

            @pl.when((s >= 2) & (s < 6) & jnp.logical_not(from_left | from_right))
            def _():
                late[...] = (mine[...] + late[...].astype(jnp.float32)).astype(jnp.bfloat16)

            @pl.when(dist == 1)
            def _():
                _send(late, tile(6, r * tiles + t), ring_s.at[s, t], end_left_r.at[r, t], right).start()

            @pl.when(dist == 3)
            def _():
                _send(late, tile(7, r * tiles + t), ring_s.at[s, t], end_right_r.at[r, t], left).start()

            @pl.when(dist == 0)
            def _():
                a, c = tile(6, r * tiles + t), tile(7, r * tiles + t)
                _send(a, a, give_s.at[0, b], end_left_r.at[r, t], right).wait_recv()
                _send(c, c, give_s.at[0, b], end_right_r.at[r, t], left).wait_recv()
                summed = mine[...] + late[...].astype(jnp.float32) + a[...].astype(jnp.float32) + c[...].astype(jnp.float32)
                for u in range(half // piece):
                    for side in range(2):
                        here = (pl.ds(pl.multiple_of((2 * u + r) * piece, piece), piece),
                                pl.ds(pl.multiple_of(t * TILE + side * fold, fold), fold))
                        part = summed[side * half + u * piece : side * half + (u + 1) * piece]
                        xr[here] = (xr[here].astype(jnp.float32) + part).astype(jnp.bfloat16)
                    y_copy(r, t, u).start()

        def turn(j, _):
            @pl.when(j < end)
            def _():
                product(j)

            @pl.when(j >= first + lag)
            def _():
                for b in range(2):
                    add(j - lag, b)

        lax.fori_loop(first, end + lag, turn, None)

        @pl.when(phase == 0)
        def _():
            project(7, True, False)
            for k in (4, 5):
                pass_out(k)
            for peer in peers:
                pl.semaphore_signal(free_late, inc=1, device_id={"tp": peer}, device_id_type=pl.DeviceIdType.MESH)
            x_load.wait()

    def y_copy(r, t, u):
        here = (pl.ds(pl.multiple_of((2 * u + r) * piece, piece), piece), pl.ds(pl.multiple_of(t * TILE, TILE), TILE))
        return pltpu.make_async_copy(xr.at[here], y_ref.at[here], y_sem.at[r, t, u])

    lax.fori_loop(0, 10, step, None)

    def finish(t, _):
        for s in range(6):
            _send(give.at[0, 0], give.at[0, 0], ring_s.at[s, t], give_r.at[0, t], right).wait_send()
        for r in range(2):
            for u in range(2):
                y_copy(r, t, u).wait()

    lax.fori_loop(0, tiles, finish, None)
    for out in range(GIVES):
        for b in range(2):
            give_copy(out, b, give.at[out, b], give_r.at[0, 0]).wait_send()


def _turns(chip_rows, chips):
    half, piece = HEAD // 2, chip_rows // 8
    freq = np.float32(THETA) ** (-np.arange(half, dtype=np.float32) / np.float32(half))
    place = np.arange(chip_rows * chips).reshape(chips, CORES, 2, 2, piece).transpose(0, 3, 1, 2, 4).reshape(-1)
    angle = (place.astype(np.float32)[:, None] * freq).astype(np.float64)
    return np.concatenate([np.cos(angle), np.sin(angle)], 1).astype(np.float32)


def solution(mesh):
    def step(x, gain, wq, wk, wv, wo):
        rows, d = x.shape
        n = mesh.shape["tp"]
        tokens = n * rows
        heads = wq.shape[1] // HEAD
        half, tiles = rows // 2, d // TILE
        bf16, f32 = jnp.bfloat16, jnp.float32
        any_, vmem, dma = pl.BlockSpec(memory_space=pl.ANY), pl.BlockSpec(memory_space=pltpu.VMEM), pltpu.SemaphoreType.DMA
        regular = pltpu.SemaphoreType.REGULAR
        return pl.pallas_call(
            _attention,
            out_shape=jax.ShapeDtypeStruct((rows, d), bf16),
            in_specs=[any_, vmem, any_, any_, any_, any_, any_],
            out_specs=any_,
            scratch_shapes=[
                pltpu.VMEM((n * rows, d), bf16),
                pltpu.VMEM(((heads + 1) * HEAD // WIDE, d, WIDE), bf16),
                pltpu.VMEM((d, HEAD), bf16),
                pltpu.VMEM((tokens, HEAD), f32),
                pltpu.VMEM((heads + 1, tokens, HEAD), bf16),
                pltpu.VMEM((tokens, HEAD), bf16),
                pltpu.VMEM((HEAD + 16, tokens), bf16),
                pltpu.VMEM((heads, rows, HEAD), bf16),
                pltpu.VMEM((2, rows, heads * HEAD), bf16),
                pltpu.VMEM((heads, HEAD + 16, rows), f32),
                pltpu.VMEM((8, rows), f32),
                pltpu.VMEM((SLOTS, 2, rows, TILE // 2), f32),
                pltpu.VMEM((GIVES, 2, rows, TILE // 2), bf16),
                pltpu.VMEM((rows, d), bf16),
                dma((4, 2)), dma((8,)), dma((2,)), dma, dma((2, tiles, 2)),
                dma((6, 2)), dma((6, 2)), dma((6, 2)), dma((6, 2)), dma((4, 2)), dma((4, 2)), dma((2, 6, 2)), dma((2, 6, 2)),
                regular, regular,
                dma((GIVES, 2)), dma((8, tiles)), dma((6, tiles)),
                dma((2, tiles // 2)), dma((2, tiles // 2)), dma((2, tiles)), dma((2, tiles)),
            ],
            compiler_params=pltpu.CompilerParams(collective_id=0, has_side_effects=True, vmem_limit_bytes=VMEM),
            name="attention",
        )(x, gain, jnp.asarray(_turns(CORES * rows, n // CORES)), wq, wk, wv, wo)

    tokens, columns = P(("dp", "tp"), None), P(None, "tp")
    return jax.shard_map(
        step,
        mesh=mesh,
        in_specs=(tokens, P(None), columns, columns, columns, P("tp", None)),
        out_specs=tokens,
        check_vma=False,
    )
```

```python
import functools

import jax
import jax.numpy as jnp
import numpy as np
from jax import lax
from jax.experimental import pallas as pl
from jax.experimental.pallas import tpu as pltpu
from jax.sharding import PartitionSpec as P

HEAD = 128
THETA = 10000
NEG = -1e30
HIDDEN = 2 * NEG
LOG2E = 1.4426950408889634
VMEM = 67043328
CORES = 2
CHIPS = 4
WIDE = 256
TILE = 512
KEYS = 512
LAG = 2
SLOTS = 3
GIVES = 4


def _dot(a, b, ca, cb):
    return lax.dot_general(a, b, (((ca,), (cb,)), ((), ())), preferred_element_type=jnp.float32)


def _places():
    me = lax.axis_index("tp")
    chip, core = me // CORES, lax.rem(me, CORES)
    right = lax.rem(chip + 1, CHIPS) * CORES + core
    left = lax.rem(chip + CHIPS - 1, CHIPS) * CORES + core
    return chip, core, right, left, chip * CORES + 1 - core


def _greet(peers):
    barrier = pltpu.get_barrier_semaphore()
    for peer in peers:
        pl.semaphore_signal(barrier, inc=1, device_id={"tp": peer}, device_id_type=pl.DeviceIdType.MESH)
    return lambda: pl.semaphore_wait(barrier, len(peers))


def _send(src, dst, send_sem, recv_sem, device):
    return pltpu.make_async_remote_copy(src_ref=src, dst_ref=dst, send_sem=send_sem, recv_sem=recv_sem, device_id={"tp": device},
                                        device_id_type=pl.DeviceIdType.MESH)


def _attention(x_ref, gain_ref, trig_ref, wq_ref, wk_ref, wv_ref, wo_ref, y_ref, xs, w, w_last, trig, qk, v, vt, qs, seen, mix, top, own, give,
               xr, x_sem, w_sem, wo_sem, xr_sem, y_sem, right_s, right_r, left_s, left_r, own_s, own_r, pass_s, pass_r, free_early,
               free_late, give_s, give_r, ring_s, through_left_r, through_right_r, end_left_r, end_right_r):
    chip, core, right, left, partner = _places()
    peers = (right, left, partner)
    ready = _greet(peers)
    rows, d = x_ref.shape
    piece, half = rows // 4, rows // 2
    heads = qs.shape[0]
    tiles = d // TILE
    mid = tiles // 2
    fold = TILE // 2
    e = HEAD**-0.5 * LOG2E

    stripe = piece // 2

    def at(group, slot, b):
        return xs.at[pl.ds(pl.multiple_of(group * rows + slot * piece + b * stripe, stripe), stripe)]

    in_turn = [(p, b) for p in (0, 1) for b in range(2)]
    in_turn = [(p + 2 * side, b) for p, b in in_turn for side in range(2)]
    loads = {
        (p, b): pltpu.make_async_copy(x_ref.at[pl.ds(p * piece + b * stripe, stripe)], at(core, p, b), x_sem.at[p, b])
        for p, b in in_turn
    }
    for f in loads.values():
        f.start()
    n_q = wq_ref.shape[1]
    n_last = n_q // WIDE
    blocks = [(wq_ref.at[:, n * WIDE : (n + 1) * WIDE], w.at[n]) for n in range(n_last)]
    blocks.append((wk_ref, w.at[n_last, :, :HEAD]))
    blocks.append((wv_ref, w.at[n_last, :, HEAD:]))
    blocks.append((wq_ref.at[:, n_last * WIDE :], w_last))
    blocks.append((trig_ref, trig))
    fetches = [pltpu.make_async_copy(a, b, w_sem.at[n]) for n, (a, b) in enumerate(blocks)]

    gain = gain_ref[...].reshape(1, d).astype(jnp.float32)

    def norm(p, b):
        def body(i, _):
            here = pl.ds(pl.multiple_of(core * rows + p * piece + b * stripe + i * 16, 16), 16)
            wide = xs[here, :].astype(jnp.float32)
            scale = lax.rsqrt(jnp.mean(wide * wide, -1, keepdims=True) + 1e-6)
            xs[here, :] = (wide * scale * gain).astype(jnp.bfloat16)

        lax.fori_loop(0, stripe // 16, body, None)

    def go_right(k, b, src):
        return _send(src, at(2 + k, 2 * core, b), right_s.at[k, b], right_r.at[k, b], right)

    def go_left(k, b, src):
        return _send(src, at(2 + k, 2 * core + 1, b), left_s.at[k, b], left_r.at[k, b], left)

    def over_own(p, b):
        return _send(at(core, p, b), at(core, p, b), own_s.at[p, b], own_r.at[p, b], partner)

    def over(k, side, b):
        here = at(2 + k, 2 * core + side, b)
        return _send(here, here, pass_s.at[side, k, b], pass_r.at[side, k, b], partner)

    def own_right(k, b):
        return go_right(k, b, at(core, k, b))

    def own_left(k, b):
        return go_left(k, b, at(core, (k + 2) % 4, b))

    for i, (p, b) in enumerate(in_turn):
        loads[p, b].wait()
        norm(p, b)
        if i == 0:
            ready()
        if p < 2:
            own_right(p, b).start()
        else:
            own_left(p - 2, b).start()
        over_own(p, b).start()
    for k in (2, 3):
        for b in range(2):
            own_right(k, b).start()
            own_left(k, b).start()
    x_load = pltpu.make_async_copy(x_ref, xr, xr_sem)
    for f in fetches:
        f.start()
    for f in fetches:
        f.wait()
    x_load.start()

    def place(group, slot):
        k = group - 2
        c, side = slot // 2, slot % 2
        near = lax.rem(chip + (1 if side else CHIPS - 1), CHIPS)
        near_part = lax.rem(k + 2, 4) if side else k
        far_part = k - 4 + 2 * side
        to = jnp.where(group < 2, chip, jnp.where(group < 6, near, lax.rem(chip + 2, CHIPS)))
        c = jnp.where(group < 2, group, c)
        part = jnp.where(group < 2, slot, jnp.where(group < 6, near_part, far_part))
        return pl.multiple_of(to * CORES * rows + lax.rem(part, 2) * rows + c * half + part // 2 * piece, piece)

    def project(group, queries, keys):
        places = [place(group, s) for s in range(4)]
        lane = lax.broadcasted_iota(jnp.int32, (piece, HEAD), 1)
        a_ref = xs.at[pl.ds(pl.multiple_of(group * rows, rows), rows)]

        def turned(both, first, count):
            for s in range(4):
                t = trig[pl.ds(places[s], piece), :]
                swapped = pltpu.roll(t, HEAD // 2, 1)
                cos = jnp.where(lane < HEAD // 2, t, swapped)
                sin = jnp.where(lane < HEAD // 2, -swapped, t)
                for h in range(count):
                    a = both[s * piece : (s + 1) * piece, h * HEAD : (h + 1) * HEAD].astype(jnp.float32)
                    qk[first + h, pl.ds(places[s], piece), :] = (a * cos + pltpu.roll(a, HEAD // 2, 1) * sin).astype(jnp.bfloat16)

        def columns(n, _):
            turned(_dot(a_ref[...], w[n], 1, 0).astype(jnp.bfloat16), n * (WIDE // HEAD), WIDE // HEAD)

        if keys:
            both = _dot(a_ref[...], w[n_last], 1, 0).astype(jnp.bfloat16)
            turned(both, heads, 1)
            for s in range(4):
                v[pl.ds(places[s], piece), :] = both[s * piece : (s + 1) * piece, HEAD:]
        if queries:
            lax.fori_loop(0, n_last, columns, None)
            turned(_dot(a_ref[...], w_last[...], 1, 0).astype(jnp.bfloat16), heads - 1, 1)

    def arrive(k):
        for b in range(2):
            go_right(k, b, at(2 + k, 2 * core, b)).wait_recv()
            over(k, 0, b).start()

            @pl.when(k < 2)
            def _():
                go_right(4 + k, b, at(2 + k, 2 * core, b)).start()

            go_left(k, b, at(2 + k, 2 * core + 1, b)).wait_recv()
            over(k, 1, b).start()

            @pl.when(k < 2)
            def _():
                go_left(4 + k, b, at(2 + k, 2 * core + 1, b)).start()

    def pass_in(k):
        for b in range(2):
            for side in range(2):
                over(k, side, b).wait_recv()

    def pass_out(k):
        for b in range(2):
            for side in range(2):
                over(k, side, b).wait_send()

    def turn(i, _):
        @pl.when(i == 1)
        def _():
            for p in range(4):
                for b in range(2):
                    here = at(1 - core, p, b)
                    _send(here, here, own_s.at[p, b], own_r.at[p, b], partner).wait_recv()

        @pl.when(i >= 2)
        def _():
            arrive(i - 2)
            pass_in(i - 2)

        project(jnp.where(i == 0, core, jnp.where(i == 1, 1 - core, i)), True, True)

    lax.fori_loop(0, 7, turn, None)

    def stage(s):
        edge = (s < 2) | (s >= 6)
        dist = jnp.where(s < 2, 2, jnp.where(s >= 6, 0, jnp.where(lax.rem(s, 2) == 0, 1, 3)))
        return dist, jnp.where(edge, lax.rem(s, 2), (s - 2) // 2)

    def block(start, keys, level):
        here = pl.ds(pl.multiple_of(start, keys), keys)
        k = qk[heads, here, :]
        values = vt[:, here]
        scores = [_dot(k, qs[h], 1, 1) for h in range(heads)]
        if level is not None:
            row = lax.broadcasted_iota(jnp.int32, (keys, rows), 0)
            lane = lax.broadcasted_iota(jnp.int32, (keys, rows), 1)
            key = row + (row // piece) * piece
            query_core = jnp.where(lane < half, 1 - core, core)
            inner = lax.rem(lane, half)
            query = query_core * rows + inner + (inner // piece) * piece
            ok = query + level * piece >= key
        weights, keeps = [], []
        for h, sc in enumerate(scores):
            if level is not None:
                sc = jnp.where(ok, sc, HIDDEN)
            old = top[h : h + 1, :]
            new = jnp.maximum(old, sc.max(axis=0, keepdims=True))
            top[h : h + 1, :] = new
            weights.append(jnp.exp2((sc - new) * e).astype(jnp.bfloat16))
            keeps.append(jnp.exp2((old - new) * e))
        for h, (p, keep) in enumerate(zip(weights, keeps)):
            mix[h] = mix[h] * keep + _dot(values, p, 1, 0)

    def attend_first(s):
        dist, r = stage(s)
        base = lax.rem(chip + dist, CHIPS) * (CORES * rows)
        for h in range(heads):
            for i, c in enumerate((1 - core, core)):
                qs[h, i * half : (i + 1) * half, :] = qk[h, pl.ds(pl.multiple_of(base + r * rows + c * half, half), half), :]
        top[...] = jnp.full(top.shape, NEG, jnp.float32)
        mix[...] = jnp.zeros(mix.shape, jnp.float32)
        lax.fori_loop(0, base // KEYS, lambda j, _: block(j * KEYS, KEYS, None), None)
        block(base, rows, r)

    def attend_last(s, seen):
        dist, r = stage(s)
        base = lax.rem(chip + dist, CHIPS) * (CORES * rows)
        block(base + rows, rows, r - 1)
        for h in range(heads):
            seen[:, h * HEAD : (h + 1) * HEAD] = (mix[h, :HEAD, :] * (1 / mix[h, HEAD : HEAD + 1, :])).T.astype(jnp.bfloat16)

    def turn_values(j):
        here = pl.ds(pl.multiple_of(j * rows, rows), rows)
        vt[:HEAD, here] = v[here, :].T

    last = lax.rem(chip + 2, CHIPS) * CORES + 1
    vt[HEAD:, :] = jnp.ones((vt.shape[0] - HEAD, vt.shape[1]), vt.dtype)
    lax.fori_loop(1, CHIPS * CORES, lambda j, _: turn_values(lax.rem(last + j, CHIPS * CORES)), None)

    for k in (2, 3):
        pass_out(k)
    for peer in peers:
        pl.semaphore_signal(free_early, inc=1, device_id={"tp": peer}, device_id_type=pl.DeviceIdType.MESH)
    attend_first(0)

    arrive(5)
    for b in range(2):
        for k in range(6):
            go_right(k, b, at(core, 0, b)).wait_send()
            go_left(k, b, at(core, 0, b)).wait_send()
        for p in range(4):
            over_own(p, b).wait_send()
    for k in (0, 1):
        pass_out(k)
    depth = wo_ref.shape[0]
    wo_loads = []
    for n in range(2):
        here = pl.ds(n * mid * TILE, mid * TILE)
        wo_loads.append(pltpu.make_async_copy(wo_ref.at[:, here], xs.at[pl.ds(0, depth), here], wo_sem.at[n]))
        wo_loads[n].start()
    pass_in(5)
    project(7, False, True)
    turn_values(last)

    def tile(group, n):
        return xs.at[pl.ds(pl.multiple_of(group * rows, rows), rows), pl.ds(pl.multiple_of(n * fold, fold), fold)]

    def ring_tile(s, t):
        n = jnp.maximum(s - 2, 0) * tiles + t
        per = w.shape[1] // rows
        return tile(5, jnp.minimum(s, 1) * tiles + t), w.at[1 + n // per, pl.ds(pl.multiple_of(lax.rem(n, per) * rows, rows), rows), :]

    def late_pair(s, pair):
        n = (s - 2) * tiles + 2 * pair
        per = w.shape[1] // rows
        return w.at[1 + n // per, pl.ds(pl.multiple_of(lax.rem(n, per) * rows, rows), 2 * rows), :]

    def end_pair(side, r, pair, b=None):
        here = pl.ds(pl.multiple_of(((side * 2 + r) * (tiles // 2) + pair) * fold, fold), fold)
        return xs.at[pl.ds(6 * rows + (b or 0) * rows, 2 * rows if b is None else rows), here]

    def folded(a):
        return jnp.concatenate([a[:, :fold], a[:, fold:]], axis=0)

    def give_copy(slot, side, dst, sem):
        return _send(give.at[slot, side], dst, give_s.at[slot, side], sem, partner)

    pairs = tiles // 2
    some = pairs // 2

    def step(phase, _):
        again = (phase == 4) | (phase == 5)
        s = jnp.where(phase < 4, phase, phase - 2)
        dist, r = stage(s)
        first = jnp.where(again, some, 0)
        end = jnp.where((phase == 2) | (phase == 3), some, pairs)
        done = jnp.where(phase < 2, phase * pairs, jnp.where(phase < 4, 2 * pairs + (phase - 2) * some, jnp.where(
            phase < 6, 2 * pairs + 2 * some + (phase - 4) * (pairs - some), (phase - 2) * pairs)))
        lag = jnp.where(phase == 0, 1, LAG)
        mine_seen = seen.at[jnp.where((phase == 3) | (phase == 5), 1, 0)]

        @pl.when((phase > 0) & jnp.logical_not(again))
        def _():
            attend_first(s)

        @pl.when(jnp.logical_not(again))
        def _():
            attend_last(s, mine_seen)

        @pl.when(phase == 0)
        def _():
            for f in wo_loads:
                f.wait()
            pl.semaphore_wait(free_early, len(peers))

        @pl.when(phase == 2)
        def _():
            pl.semaphore_wait(free_late, len(peers))

        def order(j):
            both = lax.rem(lax.rem(j, 2) * (some + 1) + j // 2, pairs)
            return jnp.where(dist == 1, lax.rem(j + some + 1, pairs), jnp.where(dist == 3, j, both))

        def product(j):
            n = done + j - first
            pair = order(j)
            both = _dot(mine_seen[...], xs[pl.ds(0, depth), pl.ds(pl.multiple_of(pair * 2 * TILE, 2 * TILE), 2 * TILE)], 1, 0)
            slot, out = lax.rem(n, SLOTS), lax.rem(n, GIVES)

            @pl.when(n >= GIVES)
            def _():
                for b in range(2):
                    give_copy(out, b, give.at[out, b], give_r.at[s, 2 * pair + b]).wait_send()

            for b in range(2):
                t = 2 * pair + b
                give[out, b] = folded(both[:half, b * TILE : (b + 1) * TILE].astype(jnp.bfloat16))
                own[slot, b] = folded(both[half:, b * TILE : (b + 1) * TILE])
                early, late = ring_tile(s, t)

                @pl.when(s < 2)
                def _():
                    give_copy(out, b, early, give_r.at[s, t]).start()

                @pl.when(s >= 2)
                def _():
                    give_copy(out, b, late, give_r.at[s, t]).start()

        def add(j, b):
            n = done + j - first
            t = 2 * order(j) + b
            give_copy(0, b, give.at[0, b], give_r.at[s, t]).wait_recv()
            mine = own.at[lax.rem(n, SLOTS), b]
            early, late = ring_tile(s, t)

            @pl.when(s < 2)
            def _():
                early[...] = (mine[...] + early[...].astype(jnp.float32)).astype(jnp.bfloat16)

                @pl.when(t < mid)
                def _():
                    _send(early, tile(4, r * tiles + t), ring_s.at[s, t], through_left_r.at[r, t], right).start()

                @pl.when(t >= mid)
                def _():
                    _send(early, tile(4, r * tiles + t), ring_s.at[s, t], through_right_r.at[r, t - mid], left).start()

            from_left = (dist == 1) & (t < mid)
            from_right = (dist == 3) & (t >= mid)
            got = tile(4, r * tiles + t)

            @pl.when(from_left)
            def _():
                _send(got, got, give_s.at[0, b], through_left_r.at[r, t], right).wait_recv()

            @pl.when(from_right)
            def _():
                _send(got, got, give_s.at[0, b], through_right_r.at[r, t - mid], left).wait_recv()

            @pl.when(from_left | from_right)
            def _():
                late[...] = (mine[...] + late[...].astype(jnp.float32) + got[...].astype(jnp.float32)).astype(jnp.bfloat16)

            @pl.when((s >= 2) & (s < 6) & jnp.logical_not(from_left | from_right))
            def _():
                late[...] = (mine[...] + late[...].astype(jnp.float32)).astype(jnp.bfloat16)

            @pl.when(dist == 0)
            def _():
                pair = order(j)
                if b == 0:
                    a, c = end_pair(0, r, pair), end_pair(1, r, pair)
                    _send(a, a, give_s.at[0, b], end_left_r.at[r, pair], right).wait_recv()
                    _send(c, c, give_s.at[0, b], end_right_r.at[r, pair], left).wait_recv()
                a, c = end_pair(0, r, pair, b), end_pair(1, r, pair, b)
                summed = mine[...] + late[...].astype(jnp.float32) + a[...].astype(jnp.float32) + c[...].astype(jnp.float32)
                for u in range(half // piece):
                    for side in range(2):
                        here = (pl.ds(pl.multiple_of((2 * u + r) * piece, piece), piece),
                                pl.ds(pl.multiple_of(t * TILE + side * fold, fold), fold))
                        part = summed[side * half + u * piece : side * half + (u + 1) * piece]
                        xr[here] = (xr[here].astype(jnp.float32) + part).astype(jnp.bfloat16)
                    y_copy(r, t, u).start()

        def turn(j, _):
            @pl.when(j < end)
            def _():
                product(j)

            @pl.when(j >= first + lag)
            def _():
                for b in range(2):
                    add(j - lag, b)
                pair = order(j - lag)

                @pl.when(dist == 1)
                def _():
                    _send(late_pair(s, pair), end_pair(0, r, pair), ring_s.at[s, pair], end_left_r.at[r, pair], right).start()

                @pl.when(dist == 3)
                def _():
                    _send(late_pair(s, pair), end_pair(1, r, pair), ring_s.at[s, pair], end_right_r.at[r, pair], left).start()

        lax.fori_loop(first, end + lag, turn, None)

        @pl.when(phase == 0)
        def _():
            project(7, True, False)
            for k in (4, 5):
                pass_out(k)
            for peer in peers:
                pl.semaphore_signal(free_late, inc=1, device_id={"tp": peer}, device_id_type=pl.DeviceIdType.MESH)
            x_load.wait()

    def y_copy(r, t, u):
        here = (pl.ds(pl.multiple_of((2 * u + r) * piece, piece), piece), pl.ds(pl.multiple_of(t * TILE, TILE), TILE))
        return pltpu.make_async_copy(xr.at[here], y_ref.at[here], y_sem.at[r, t, u])

    lax.fori_loop(0, 10, step, None)

    def finish(t, _):
        for s in range(2):
            _send(give.at[0, 0], give.at[0, 0], ring_s.at[s, t], give_r.at[0, t], right).wait_send()

        @pl.when(t < pairs)
        def _():
            for s in range(2, 6):
                _send(late_pair(s, 0), late_pair(s, 0), ring_s.at[s, t], give_r.at[0, t], right).wait_send()

        for r in range(2):
            for u in range(2):
                y_copy(r, t, u).wait()

    lax.fori_loop(0, tiles, finish, None)
    for out in range(GIVES):
        for b in range(2):
            give_copy(out, b, give.at[out, b], give_r.at[0, 0]).wait_send()


def _hand_on(a_ref, b_ref, held, in_sem, out_sem):
    n, rows = held.shape[:2]
    here = [pl.ds(i * rows, rows) for i in range(n)]
    ins = [pltpu.make_async_copy(a_ref.at[here[i]], held.at[i], in_sem.at[i]) for i in range(n)]
    outs = [pltpu.make_async_copy(held.at[i], b_ref.at[here[i]], out_sem.at[i]) for i in range(n)]
    for f in ins:
        f.start()
    for i in range(n):
        ins[i].wait()
        outs[i].start()
    for f in outs:
        f.wait()


def _turns(chip_rows, chips):
    half, piece = HEAD // 2, chip_rows // 8
    freq = np.float32(THETA) ** (-np.arange(half, dtype=np.float32) / np.float32(half))
    place = np.arange(chip_rows * chips).reshape(chips, CORES, 2, 2, piece).transpose(0, 3, 1, 2, 4).reshape(-1)
    angle = (place.astype(np.float32)[:, None] * freq).astype(np.float64)
    return np.concatenate([np.cos(angle), np.sin(angle)], 1).astype(np.float32)


def solution(mesh):
    def step(x, gain, wq, wk, wv, wo):
        rows, d = x.shape
        n = mesh.shape["tp"]
        tokens = n * rows
        heads = wq.shape[1] // HEAD
        half, tiles = rows // 2, d // TILE
        bf16, f32 = jnp.bfloat16, jnp.float32
        any_, vmem, dma = pl.BlockSpec(memory_space=pl.ANY), pl.BlockSpec(memory_space=pltpu.VMEM), pltpu.SemaphoreType.DMA
        regular = pltpu.SemaphoreType.REGULAR
        y = pl.pallas_call(
            _attention,
            out_shape=jax.ShapeDtypeStruct((rows, d), bf16),
            in_specs=[any_, vmem, any_, any_, any_, any_, any_],
            out_specs=any_,
            scratch_shapes=[
                pltpu.VMEM((n * rows, d), bf16),
                pltpu.VMEM(((heads + 1) * HEAD // WIDE, d, WIDE), bf16),
                pltpu.VMEM((d, HEAD), bf16),
                pltpu.VMEM((tokens, HEAD), f32),
                pltpu.VMEM((heads + 1, tokens, HEAD), bf16),
                pltpu.VMEM((tokens, HEAD), bf16),
                pltpu.VMEM((HEAD + 16, tokens), bf16),
                pltpu.VMEM((heads, rows, HEAD), bf16),
                pltpu.VMEM((2, rows, heads * HEAD), bf16),
                pltpu.VMEM((heads, HEAD + 16, rows), f32),
                pltpu.VMEM((8, rows), f32),
                pltpu.VMEM((SLOTS, 2, rows, TILE // 2), f32),
                pltpu.VMEM((GIVES, 2, rows, TILE // 2), bf16),
                pltpu.VMEM((rows, d), bf16),
                dma((4, 2)), dma((8,)), dma((2,)), dma, dma((2, tiles, 2)),
                dma((6, 2)), dma((6, 2)), dma((6, 2)), dma((6, 2)), dma((4, 2)), dma((4, 2)), dma((2, 6, 2)), dma((2, 6, 2)),
                regular, regular,
                dma((GIVES, 2)), dma((8, tiles)), dma((6, tiles)),
                dma((2, tiles // 2)), dma((2, tiles // 2)), dma((2, tiles // 2)), dma((2, tiles // 2)),
            ],
            compiler_params=pltpu.CompilerParams(collective_id=0, has_side_effects=True, vmem_limit_bytes=VMEM),
            name="attention",
        )(x, gain, jnp.asarray(_turns(CORES * rows, n // CORES)), wq, wk, wv, wo)
        return pl.pallas_call(
            _hand_on,
            out_shape=jax.ShapeDtypeStruct((rows, d), bf16),
            in_specs=[any_],
            out_specs=any_,
            scratch_shapes=[pltpu.VMEM((8, rows // 8, d), bf16), dma((8,)), dma((8,))],
            name="hand_on",
        )(y)

    tokens, columns = P(("dp", "tp"), None), P(None, "tp")
    return jax.shard_map(
        step,
        mesh=mesh,
        in_specs=(tokens, P(None), columns, columns, columns, P("tp", None)),
        out_specs=tokens,
        check_vma=False,
    )
```
